32 devices in a mesh: group: 2 (over x), lat: 16 (over z, y, core).
Axes of the slice: x: 2, y: 2, z: 4, core: 2. Of those that a mesh axis runs over, the one named last changes fastest.
Arguments:
- grid_values: bfloat16 [224, 1440, 256], P(('group', 'lat')), parts along dimension 0, may hold values from -630 to 630
- lat_counts: int32 [16], replicated, may hold values from 1 to 7, 96 in all
- owner_wavenumber: int32 [384], replicated, may hold values from 0 to 383, each once
- legendre: bfloat16 [384, 96, 384], P('lat'), may hold values from -0.625 to 0.625
- quad_weight: float32 [96], replicated, may hold values from 0.3 to 3
- spectral_gain: float32 [384, 256], replicated, may hold values from 0.3 to 3
- channel_mix: bfloat16 [256, 256], replicated, may hold values from -0.375 to 0.375
Outputs:
- grid_output: bfloat16 [224, 1440, 256], P(('group', 'lat')), parts along dimension 0
The draws below stay inside these ranges and needn't reach their ends.
There are 2 independent parts, one for each index of `group`. The reference program is written for one: setup_inputs(seed, part) draws one part's arguments, and reference() takes and returns one part's arrays. A program takes and returns all parts, laid end to end along the dimension named above; an argument that names none is the same for every part. Nothing has to cross between parts.
Inputs may be any that keep to these rules, and one draw needn't show every extreme that they name: `lat_counts`: some device has all 7 slots live. `owner_wavenumber`: each wavenumber appears once; device i of lat owns wavenumber slots i * 24 to (i + 1) * 24 - 1.
All inputs are finite; a program needn't handle non-finite values.
Results may differ from the reference program's by a relative error of at most 0.0095.
Values may be sent and summed in bfloat16 or wider, within the bound.
A program may use at most 64 MiB of HBM per device.

```python
import math
import jax
import jax.numpy as jnp
import numpy as np
from jax import lax

LONGITUDES = 1440
CHANNELS = 256
WAVES = 384
DEGREES = 384
LAT_SLOTS = 7
SLOTS_ALL = 112
LIVE_LATS = 96
N_LAT = 16


def draw_grid_values(key, part):
    key_rows = jax.random.fold_in(key, 11)
    key_scale = jax.random.fold_in(key, 12)
    key_mean = jax.random.fold_in(key, 13)
    key_noise = jax.random.fold_in(key, 14)
    position = jnp.arange(SLOTS_ALL, dtype=jnp.float32) / SLOTS_ALL
    jitter = jax.random.uniform(key_rows, (SLOTS_ALL,), minval=-0.1, maxval=0.1)
    row_scale = jnp.exp(jnp.log(10.0) * jnp.clip(position + jitter, 0.0, 1.0))
    chan_scale = jnp.exp(jax.random.uniform(key_scale, (CHANNELS,), minval=0.0, maxval=jnp.log(10.0)))
    chan_mean = jax.random.uniform(key_mean, (CHANNELS,), minval=-1.0, maxval=1.0)
    noise = jnp.clip(jax.random.normal(key_noise, (SLOTS_ALL, LONGITUDES, CHANNELS)), -6.0, 6.0)
    values = chan_mean[None, None, :] * chan_scale[None, None, :] + row_scale[:, None, None] * chan_scale[None, None, :] * noise
    return values.astype(jnp.float32).astype(jnp.bfloat16)


def block_levels(rng, shape, cuts, low, top_value):
    loudness, own = 1.0, jax.random.fold_in(rng, 6)
    for dim, blocks in cuts:
        heights = jnp.exp(jax.random.uniform(jax.random.fold_in(own, dim), (blocks,), jnp.float32, low / len(cuts), top_value / len(cuts)))
        loudness = loudness * jnp.repeat(heights, shape[dim] // blocks).reshape([-1 if axis == dim else 1 for axis in range(len(shape))])
    return loudness


def length_profile(number_of, total, reach, lean):
    weights = [(1 << 20) // math.isqrt(rank ** lean) + 1 for rank in range(2, number_of + 1)]
    spare, given = total - reach - (number_of - 1), [1] * (number_of - 1)
    while spare > 0:
        movable = [i for i in range(number_of - 1) if given[i] < reach]
        mass, budget = sum([weights[i] for i in movable]), spare
        for i in movable:
            extra = min(reach - given[i], max(1, budget * weights[i] // mass), spare)
            given[i] = given[i] + extra
            spare = spare - extra
    return np.array([reach] + given)


def ragged(key, amount, total, bound, slope):
    if amount == 2:
        one = jax.random.randint(key, (), max(1, total - bound), min(bound, total - 1) + 1)
        return jnp.stack([one, total - one])
    lengths = jnp.asarray(length_profile(amount, total, bound, slope), jnp.int32)
    pairs = (amount - 1) // 2
    giver, sink = lengths[1:1 + 2 * pairs:2], lengths[2:2 + 2 * pairs:2]
    room = jnp.minimum(giver - 1, bound - sink)
    shifted = jax.random.randint(jax.random.fold_in(key, 1), (pairs,), 0, 1 << 20) % (room + 1)
    lengths = lengths.at[1:1 + 2 * pairs:2].set(giver - shifted).at[2:2 + 2 * pairs:2].set(sink + shifted)
    return lengths[jax.random.permutation(jax.random.fold_in(key, 2), amount)]


def scatter_about(rng, extent, spread, limit, split=(), held_as=jnp.bfloat16):
    level = block_levels(rng, extent, split, -0.22, 0.18) if split else 1.0
    values = jax.random.normal(rng, extent, jnp.float32) * spread * level
    return jnp.minimum(jnp.maximum(values, -limit), limit).astype(held_as)


def setup_inputs(seed: int = 0, part: int = 0) -> dict:
    splits = jax.random.split(jax.random.key(seed), 8)
    own_keys = jax.random.split(jax.random.fold_in(splits[7], part), 8)
    return {
        "grid_values": draw_grid_values(jax.random.fold_in(jax.random.fold_in(splits[7], part), 71), part),
        "lat_counts": ragged(splits[1], N_LAT, LIVE_LATS, LAT_SLOTS, 2).astype(jnp.int32),
        "owner_wavenumber": jax.random.permutation(splits[2], WAVES).astype(jnp.int32),
        "legendre": scatter_about(splits[3], (WAVES, LIVE_LATS, DEGREES), LIVE_LATS ** -0.5, 0.625, ((0, 16),)),
        "quad_weight": jnp.clip(jnp.exp(jax.random.uniform(splits[4], (LIVE_LATS,), jnp.float32, math.log(0.3), math.log(3.0))), 0.3, 3.0),
        "spectral_gain": jnp.clip(jnp.exp(jax.random.uniform(splits[5], (DEGREES, CHANNELS), jnp.float32, math.log(0.3), math.log(3.0))), 0.3, 3.0),
        "channel_mix": scatter_about(splits[6], (CHANNELS, CHANNELS), CHANNELS ** -0.5, 0.375),
    }


def live_slots(lat_counts, slot_count, live_total):
    devices = lat_counts.shape[0]
    starts = jnp.cumsum(lat_counts) - lat_counts
    device_ids = jnp.arange(devices, dtype=jnp.int32)
    slot_ids = jnp.arange(devices * slot_count, dtype=jnp.int32)
    holder = slot_ids // slot_count
    within = slot_ids - holder * slot_count
    holder_hot = holder[:, None] == device_ids[None, :]
    holder_count = lax.optimization_barrier(jnp.sum(jnp.where(holder_hot, lat_counts[None, :], 0), axis=1))
    holder_start = lax.optimization_barrier(jnp.sum(jnp.where(holder_hot, starts[None, :], 0), axis=1))
    slot_valid = within < holder_count
    slot_live = jnp.where(slot_valid, holder_start + within, 0).astype(jnp.int32)
    live_ids = jnp.arange(live_total, dtype=jnp.int32)
    reached = (starts[None, :] <= live_ids[:, None]).astype(jnp.int32)
    source = lax.optimization_barrier(jnp.sum(reached, axis=1)) - 1
    source_hot = source[:, None] == device_ids[None, :]
    source_start = lax.optimization_barrier(jnp.sum(jnp.where(source_hot, starts[None, :], 0), axis=1))
    live_slot = (source * slot_count + live_ids - source_start).astype(jnp.int32)
    return (slot_valid, slot_live, live_slot)

def wave_angles(wave_list, longitudes):
    points = jnp.arange(longitudes, dtype=jnp.int32)
    phase = wave_list[:, None] * points[None, :] % longitudes
    return phase.astype(jnp.float32) * (2.0 * math.pi / longitudes)

def forward_table(wave_list, longitudes):
    angle = wave_angles(wave_list, longitudes)
    factor = 1.0 / math.sqrt(longitudes)
    return jnp.stack([jnp.cos(angle) * factor, -jnp.sin(angle) * factor], axis=1).astype(jnp.bfloat16)

def inverse_table(wave_list, longitudes):
    angle = wave_angles(wave_list, longitudes)
    factor = 1.0 / math.sqrt(longitudes)
    doubled = jnp.where(wave_list > 0, 2.0, 1.0).astype(jnp.float32)[:, None] * factor
    return jnp.stack([jnp.cos(angle) * doubled, -jnp.sin(angle) * doubled], axis=1).astype(jnp.bfloat16)

def reference(grid_values, lat_counts, owner_wavenumber, legendre, quad_weight, spectral_gain, channel_mix):
    slot_valid, slot_live, live_slot = live_slots(lat_counts, LAT_SLOTS, LIVE_LATS)
    row_weight = slot_valid.astype(jnp.float32)[:, None, None]
    widened = grid_values.astype(jnp.float32) * row_weight
    points = LIVE_LATS * LONGITUDES
    channel_mean = lax.optimization_barrier(jnp.sum(widened, axis=(0, 1))) / points
    variance = lax.optimization_barrier(jnp.sum(widened * widened, axis=(0, 1))) / points - channel_mean * channel_mean
    normed = ((grid_values.astype(jnp.float32) - channel_mean) * lax.rsqrt(variance + 1e-05) * row_weight).astype(jnp.bfloat16)
    forward = forward_table(owner_wavenumber, LONGITUDES)
    spectra = jnp.einsum('skc,rtk->srtc', normed.astype(jnp.float32), forward.astype(jnp.float32)).astype(jnp.bfloat16)
    gathered = jnp.take(spectra, live_slot, axis=0)
    weighted = (gathered.astype(jnp.float32) * quad_weight[:, None, None, None]).astype(jnp.bfloat16)
    coefficient = jnp.einsum('rgl,grtc->rltc', legendre.astype(jnp.float32), weighted.astype(jnp.float32))
    degree_mask = (jnp.arange(DEGREES, dtype=jnp.int32)[None, :] >= owner_wavenumber[:, None]).astype(jnp.float32)
    filtered = (coefficient * degree_mask[:, :, None, None] * spectral_gain[None, :, None, :]).astype(jnp.bfloat16)
    mixed = jnp.dot(filtered.reshape(-1, CHANNELS), channel_mix, preferred_element_type=jnp.float32)
    mixed = mixed.astype(jnp.bfloat16).reshape(WAVES, DEGREES, 2, CHANNELS)
    synthesis = jnp.einsum('rgl,rltc->grtc', legendre.astype(jnp.float32), mixed.astype(jnp.float32)).astype(jnp.bfloat16)
    outgoing = jnp.where(slot_valid[:, None, None, None], jnp.take(synthesis, slot_live, axis=0), jnp.zeros((), jnp.bfloat16))
    inverse = inverse_table(owner_wavenumber, LONGITUDES)
    result = jnp.einsum('srtc,rtk->skc', outgoing.astype(jnp.float32), inverse.astype(jnp.float32))
    return result.astype(jnp.bfloat16)
```

```python
import functools
import math

import jax
import jax.numpy as jnp
import numpy as np
from jax import lax
from jax.experimental import pallas as pl
from jax.experimental.pallas import tpu as pltpu
from jax.sharding import PartitionSpec as P

BLOCK = 8
F32 = jnp.float32
BF16 = jnp.bfloat16


def trig_table(waves, longitudes):
    phase = np.arange(waves)[:, None] * np.arange(longitudes)[None, :] % longitudes
    angle = phase * (2.0 * math.pi / longitudes)
    factor = 1.0 / math.sqrt(longitudes)
    table = np.concatenate([np.cos(angle) * factor, -np.sin(angle) * factor], axis=0)
    return table.astype(BF16)


def greet_all(axis, count, me):
    barrier = pltpu.get_barrier_semaphore()

    def signal(i, carry):
        other = lax.rem(me + i, count)
        pl.semaphore_signal(
            barrier, inc=1, device_id={axis: other}, device_id_type=pl.DeviceIdType.MESH
        )
        return carry

    lax.fori_loop(1, count, signal, 0)
    return barrier


def forward_kernel(
    axis, n, points, counts, x, base, rows, recv, back_table,
    sums, table, normed, spec, mom_send, mom_recv, send, arrive, own,
):
    me = lax.axis_index(axis)
    slots = x.shape[0]
    barrier = greet_all(axis, n, me)
    live = counts[me]
    zero = jnp.zeros((1, x.shape[2]), F32)

    def add_slot(s, carry):
        first, second = carry
        wide = x[s].astype(F32)
        weight = jnp.where(s < live, 1.0, 0.0).astype(F32)
        first = first + weight * jnp.sum(wide, axis=0, keepdims=True)
        second = second + weight * jnp.sum(wide * wide, axis=0, keepdims=True)
        return first, second

    first, second = lax.fori_loop(0, slots, add_slot, (zero, zero))
    sums[me, 0:1, :] = first
    sums[me, 1:2, :] = second
    pl.semaphore_wait(barrier, n - 1)

    def moment_copy(i):
        other = lax.rem(me + i, n)
        return pltpu.make_async_remote_copy(
            src_ref=sums.at[me], dst_ref=sums.at[me],
            send_sem=mom_send.at[i], recv_sem=mom_recv.at[i],
            device_id={axis: other}, device_id_type=pl.DeviceIdType.MESH,
        )

    def start_moment(i, carry):
        moment_copy(i).start()
        return carry

    def wait_moment(i, carry):
        moment_copy(i).wait()
        return carry

    lax.fori_loop(1, n, start_moment, 0)
    total = base.shape[0]
    chosen = rows[...] == lax.broadcasted_iota(jnp.int32, (rows.shape[0], total), 1)
    chosen = jnp.where(chosen, 1.0, 0.0).astype(BF16)
    table[...] = jnp.dot(chosen, base[...], preferred_element_type=F32).astype(BF16)
    lax.fori_loop(1, n, wait_moment, 0)
    both = jnp.sum(sums[...], axis=0)
    mean = both[0:1] / points
    variance = both[1:2] / points - mean * mean
    scale = lax.rsqrt(variance + 1e-05)

    def block_copy(i, s):
        other = lax.rem(me + i, n)
        return pltpu.make_async_remote_copy(
            src_ref=spec.at[other, s], dst_ref=recv.at[me, s],
            send_sem=send.at[i], recv_sem=arrive.at[i],
            device_id={axis: other}, device_id_type=pl.DeviceIdType.MESH,
        )

    def slot_step(s, carry):
        weight = jnp.where(s < live, 1.0, 0.0).astype(F32)
        normed[...] = ((x[s].astype(F32) - mean) * scale * weight).astype(BF16)
        out = jnp.dot(table[...], normed[...], preferred_element_type=F32).astype(BF16)
        spec[:, s] = out.reshape(spec.shape[0], spec.shape[2], spec.shape[3])

        def start_block(i, inner):
            block_copy(i, s).start()
            return inner

        lax.fori_loop(1, n, start_block, 0)
        return carry

    lax.fori_loop(0, slots, slot_step, 0)
    mine = pltpu.make_async_copy(spec.at[me], recv.at[me], own)
    mine.start()
    back_table[...] = table[...].T

    def wait_block(i, carry):
        other = lax.rem(me + i, n)
        pltpu.make_async_remote_copy(
            src_ref=spec.at[other], dst_ref=recv.at[me],
            send_sem=send.at[i], recv_sem=arrive.at[i],
            device_id={axis: other}, device_id_type=pl.DeviceIdType.MESH,
        ).wait()
        return carry

    lax.fori_loop(1, n, wait_block, 0)
    mine.wait()


def middle_kernel(
    axis, n, share, counts, owner, spectra, legendre, quad, gain, mix, back,
    gathered, pick, quad_slot, outgoing, result, send, arrive, own,
):
    me = lax.axis_index(axis)
    slots, height = spectra.shape[1], spectra.shape[2]
    everything = n * slots
    live_total, degrees = legendre.shape[1], legendre.shape[2]
    channels = mix.shape[0]
    halves = channels // 128
    blocks = height // (2 * BLOCK)
    barrier = greet_all(axis, n, me)

    row = lax.broadcasted_iota(jnp.int32, (everything, live_total), 0)
    lane = lax.broadcasted_iota(jnp.int32, (everything, live_total), 1)
    pick[...] = jnp.zeros_like(pick)

    def mark(i, begin):
        within = row - i * slots
        hit = (within >= 0) & (within < counts[i]) & (lane == begin + within)
        pick[...] += jnp.where(hit, 1.0, 0.0).astype(F32)
        return begin + counts[i]

    lax.fori_loop(0, n, mark, jnp.int32(0))
    quad_slot[...] = jnp.broadcast_to(
        jnp.sum(pick[...] * quad[...], axis=1, keepdims=True), quad_slot.shape
    )

    def widen(i, carry):
        for s in range(slots):
            wide = spectra[i, s].astype(F32)
            begin = pl.multiple_of((i * slots + s) * height, 8)
            for h in range(halves):
                gathered[h, pl.ds(begin, height), :] = wide[:, h * 128 : (h + 1) * 128]
        return carry

    lax.fori_loop(0, n, widen, 0)
    degree = lax.broadcasted_iota(jnp.int32, (degrees, channels), 0)

    def block_copy(i, b):
        other = lax.rem(me + i, n)
        return pltpu.make_async_remote_copy(
            src_ref=outgoing.at[b, other],
            dst_ref=back.at[me, :, pl.ds(b * 2 * BLOCK, 2 * BLOCK), :],
            send_sem=send.at[b, i], recv_sem=arrive.at[b, i],
            device_id={axis: other}, device_id_type=pl.DeviceIdType.MESH,
        )

    def own_copy(b):
        return pltpu.make_async_copy(
            outgoing.at[b, me],
            back.at[me, :, pl.ds(b * 2 * BLOCK, 2 * BLOCK), :],
            own.at[b],
        )

    for b in range(blocks):
        count = min(BLOCK, share - b * BLOCK)
        if count < BLOCK:
            result[...] = jnp.zeros_like(result)

        def wave_step(r, carry):
            wave = owner[me * share + b * BLOCK + r]
            expanded = jnp.dot(
                pick[...].astype(BF16), legendre[b * BLOCK + r], preferred_element_type=F32
            ).astype(BF16)
            pieces = []
            for t in range(2):
                for h in range(halves):
                    start = b * 2 * BLOCK + t * BLOCK + r
                    piece = gathered[h, pl.ds(start, everything, stride=height), :]
                    pieces.append((piece * quad_slot[...]).astype(BF16))
            weighted = jnp.concatenate(pieces, axis=1)
            coefficient = lax.dot_general(
                expanded, weighted, (((0,), (0,)), ((), ())), preferred_element_type=F32
            )
            kept = degree >= wave
            factor = jnp.where(wave > 0, 2.0, 1.0).astype(F32)
            mixed = []
            for t in range(2):
                part = coefficient[:, t * channels : (t + 1) * channels] * gain[...]
                part = jnp.where(kept, part, 0.0).astype(BF16)
                mixed.append(jnp.dot(part, mix[...], preferred_element_type=F32).astype(BF16))
            synthesis = jnp.dot(
                expanded, jnp.concatenate(mixed, axis=1), preferred_element_type=F32
            ) * factor
            for t in range(2):
                for h in range(halves):
                    begin = t * channels + h * 128
                    result[h, pl.ds(t * BLOCK + r, everything, stride=2 * BLOCK), :] = synthesis[
                        :, begin : begin + 128
                    ]
            return carry

        lax.fori_loop(0, count, wave_step, 0)

        def narrow(i, carry):
            for s in range(slots):
                begin = pl.multiple_of((i * slots + s) * 2 * BLOCK, 8)
                outgoing[b, i, s] = jnp.concatenate(
                    [result[h, pl.ds(begin, 2 * BLOCK), :] for h in range(halves)], axis=1
                ).astype(BF16)
            return carry

        lax.fori_loop(0, n, narrow, 0)
        if b == 0:
            pl.semaphore_wait(barrier, n - 1)

        def start_block(i, carry):
            block_copy(i, b).start()
            return carry

        lax.fori_loop(1, n, start_block, 0)
        own_copy(b).start()

    for b in range(blocks):

        def wait_block(i, carry):
            block_copy(i, b).wait()
            return carry

        lax.fori_loop(1, n, wait_block, 0)
        own_copy(b).wait()


def inverse_kernel(back, table, out):
    block = back[...].reshape(table.shape[1], back.shape[2])
    out[0] = jnp.dot(table[...], block, preferred_element_type=F32).astype(BF16)


def body(
    n, grid_values, lat_counts, owner_wavenumber, legendre, quad_weight, spectral_gain, channel_mix
):
    slots, longitudes, channels = grid_values.shape
    waves = owner_wavenumber.shape[0]
    share, live_total, degrees = legendre.shape
    blocks = -(-share // BLOCK)
    padded = blocks * BLOCK
    height = 2 * padded
    everything = n * slots
    base = jnp.asarray(trig_table(waves, longitudes))
    slot_waves = owner_wavenumber.reshape(n, share)
    slot_waves = jnp.pad(slot_waves, ((0, 0), (0, padded - share)), constant_values=-2 * waves)
    slot_waves = slot_waves.reshape(n, blocks, 1, BLOCK)
    rows = jnp.concatenate([slot_waves, slot_waves + waves], axis=2).reshape(n * height, 1)

    vmem = pl.BlockSpec(memory_space=pltpu.VMEM)
    smem = pl.BlockSpec(memory_space=pltpu.SMEM)
    anywhere = pl.BlockSpec(memory_space=pl.ANY)
    limit = 60 * 1024 * 1024
    recv, back_table = pl.pallas_call(
        functools.partial(forward_kernel, "lat", n, live_total * longitudes),
        out_shape=(
            jax.ShapeDtypeStruct((n, slots, height, channels), BF16),
            jax.ShapeDtypeStruct((longitudes, n * height), BF16),
        ),
        in_specs=[smem, vmem, vmem, vmem],
        out_specs=(anywhere, vmem),
        scratch_shapes=[
            pltpu.VMEM((n, 2, channels), F32),
            pltpu.VMEM((n * height, longitudes), BF16),
            pltpu.VMEM((longitudes, channels), BF16),
            pltpu.VMEM((n, slots, height, channels), BF16),
            pltpu.SemaphoreType.DMA((n,)),
            pltpu.SemaphoreType.DMA((n,)),
            pltpu.SemaphoreType.DMA((n,)),
            pltpu.SemaphoreType.DMA((n,)),
            pltpu.SemaphoreType.DMA,
        ],
        compiler_params=pltpu.CompilerParams(
            collective_id=0, has_side_effects=True, vmem_limit_bytes=limit
        ),
    )(lat_counts, grid_values, base, rows)

    back = pl.pallas_call(
        functools.partial(middle_kernel, "lat", n, share),
        out_shape=jax.ShapeDtypeStruct((n, slots, height, channels), BF16),
        in_specs=[smem, smem, vmem, vmem, vmem, vmem, vmem],
        out_specs=anywhere,
        scratch_shapes=[
            pltpu.VMEM((channels // 128, everything * height, 128), F32),
            pltpu.VMEM((everything, live_total), F32),
            pltpu.VMEM((everything, 128), F32),
            pltpu.VMEM((blocks, n, slots, 2 * BLOCK, channels), BF16),
            pltpu.VMEM((channels // 128, everything * 2 * BLOCK, 128), F32),
            pltpu.SemaphoreType.DMA((blocks, n)),
            pltpu.SemaphoreType.DMA((blocks, n)),
            pltpu.SemaphoreType.DMA((blocks,)),
        ],
        compiler_params=pltpu.CompilerParams(
            collective_id=1, has_side_effects=True, vmem_limit_bytes=limit
        ),
    )(
        lat_counts, owner_wavenumber, recv, legendre, quad_weight.reshape(1, live_total),
        spectral_gain, channel_mix,
    )

    return pl.pallas_call(
        inverse_kernel,
        grid=(slots,),
        out_shape=jax.ShapeDtypeStruct((slots, longitudes, channels), BF16),
        in_specs=[
            pl.BlockSpec((n, None, height, channels), lambda s: (0, s, 0, 0)),
            pl.BlockSpec((longitudes, n * height), lambda s: (0, 0)),
        ],
        out_specs=pl.BlockSpec((1, longitudes, channels), lambda s: (s, 0, 0)),
        compiler_params=pltpu.CompilerParams(vmem_limit_bytes=limit),
    )(back, back_table)


def solution(mesh):
    return jax.shard_map(
        functools.partial(body, mesh.shape["lat"]),
        mesh=mesh,
        in_specs=(P(("group", "lat"), None, None), P(), P(), P("lat", None, None), P(), P(), P()),
        out_specs=P(("group", "lat"), None, None),
        check_vma=False,
    )
```

```python
import functools
import math

import jax
import jax.numpy as jnp
import numpy as np
from jax import lax
from jax.experimental import pallas as pl
from jax.experimental.pallas import tpu as pltpu
from jax.sharding import PartitionSpec as P

BLOCK = 8
F32 = jnp.float32
BF16 = jnp.bfloat16


def trig_table(waves, longitudes):
    phase = np.arange(waves)[:, None] * np.arange(longitudes)[None, :] % longitudes
    angle = phase * (2.0 * math.pi / longitudes)
    factor = 1.0 / math.sqrt(longitudes)
    table = np.concatenate([np.cos(angle) * factor, -np.sin(angle) * factor], axis=0)
    return table.astype(BF16)


def greet_all(axis, count, me):
    barrier = pltpu.get_barrier_semaphore()

    def signal(i, carry):
        other = lax.rem(me + i, count)
        pl.semaphore_signal(
            barrier, inc=1, device_id={axis: other}, device_id_type=pl.DeviceIdType.MESH
        )
        return carry

    lax.fori_loop(1, count, signal, 0)
    return barrier


def spectral_kernel(
    axis, n, points, share, counts, owner, x, base, rows, legendre, quad, gain, mix,
    back, back_table,
    sums, table, normed, spec, recv, gathered, pick, quad_slot, outgoing, result,
    mom_send, mom_recv, send, arrive, own, back_send, back_arrive, back_own,
):
    me = lax.axis_index(axis)
    slots, channels = x.shape[0], x.shape[2]
    everything = n * slots
    live_total, degrees = legendre.shape[1], legendre.shape[2]
    halves = channels // 128
    blocks = spec.shape[0]
    lines = n * 2 * BLOCK
    barrier = greet_all(axis, n, me)
    live = counts[me]
    zero = jnp.zeros((1, channels), F32)

    def add_slot(s, carry):
        first, second = carry
        wide = x[s].astype(F32)
        weight = jnp.where(s < live, 1.0, 0.0).astype(F32)
        first = first + weight * jnp.sum(wide, axis=0, keepdims=True)
        second = second + weight * jnp.sum(wide * wide, axis=0, keepdims=True)
        return first, second

    first, second = lax.fori_loop(0, slots, add_slot, (zero, zero))
    sums[me, 0:1, :] = first
    sums[me, 1:2, :] = second
    pl.semaphore_wait(barrier, n - 1)

    def moment_copy(i):
        other = lax.rem(me + i, n)
        return pltpu.make_async_remote_copy(
            src_ref=sums.at[me], dst_ref=sums.at[me],
            send_sem=mom_send.at[i], recv_sem=mom_recv.at[i],
            device_id={axis: other}, device_id_type=pl.DeviceIdType.MESH,
        )

    def start_moment(i, carry):
        moment_copy(i).start()
        return carry

    def wait_moment(i, carry):
        moment_copy(i).wait()
        return carry

    lax.fori_loop(1, n, start_moment, 0)
    total = base.shape[0]
    chosen = rows[...] == lax.broadcasted_iota(jnp.int32, (rows.shape[0], total), 1)
    chosen = jnp.where(chosen, 1.0, 0.0).astype(BF16)
    table[...] = jnp.dot(chosen, base[...], preferred_element_type=F32).astype(BF16)
    lax.fori_loop(1, n, wait_moment, 0)
    both = jnp.sum(sums[...], axis=0)
    mean = both[0:1] / points
    variance = both[1:2] / points - mean * mean
    scale = lax.rsqrt(variance + 1e-05)

    def block_copy(b, i):
        other = lax.rem(me + i, n)
        return pltpu.make_async_remote_copy(
            src_ref=spec.at[b, other], dst_ref=recv.at[b, me],
            send_sem=send.at[b, i], recv_sem=arrive.at[b, i],
            device_id={axis: other}, device_id_type=pl.DeviceIdType.MESH,
        )

    for b in range(blocks):

        def slot_step(s, carry):
            if b == 0:
                weight = jnp.where(s < live, 1.0, 0.0).astype(F32)
                normed[s] = ((x[s].astype(F32) - mean) * scale * weight).astype(BF16)
            out = jnp.dot(
                table[b * lines : (b + 1) * lines], normed[s], preferred_element_type=F32
            )
            spec[b, :, s] = out.astype(BF16).reshape(n, 2 * BLOCK, channels)
            if b == 0:

                def start_slot(i, inner):
                    other = lax.rem(me + i, n)
                    pltpu.make_async_remote_copy(
                        src_ref=spec.at[b, other, s], dst_ref=recv.at[b, me, s],
                        send_sem=send.at[b, i], recv_sem=arrive.at[b, i],
                        device_id={axis: other}, device_id_type=pl.DeviceIdType.MESH,
                    ).start()
                    return inner

                lax.fori_loop(1, n, start_slot, 0)
            return carry

        lax.fori_loop(0, slots, slot_step, 0)
        if b > 0:

            def start_block(i, carry):
                block_copy(b, i).start()
                return carry

            lax.fori_loop(1, n, start_block, 0)
        pltpu.make_async_copy(spec.at[b, me], recv.at[b, me], own.at[b]).start()

    back_table[...] = table[...].T
    row = lax.broadcasted_iota(jnp.int32, (everything, live_total), 0)
    lane = lax.broadcasted_iota(jnp.int32, (everything, live_total), 1)
    pick[...] = jnp.zeros_like(pick)

    def mark(i, begin):
        within = row - i * slots
        hit = (within >= 0) & (within < counts[i]) & (lane == begin + within)
        pick[...] += jnp.where(hit, 1.0, 0.0).astype(F32)
        return begin + counts[i]

    lax.fori_loop(0, n, mark, jnp.int32(0))
    quad_slot[...] = jnp.broadcast_to(
        jnp.sum(pick[...] * quad[...], axis=1, keepdims=True), quad_slot.shape
    )
    degree = lax.broadcasted_iota(jnp.int32, (degrees, channels), 0)

    def return_copy(b, i):
        other = lax.rem(me + i, n)
        return pltpu.make_async_remote_copy(
            src_ref=outgoing.at[b, other], dst_ref=back.at[b, me],
            send_sem=back_send.at[b, i], recv_sem=back_arrive.at[b, i],
            device_id={axis: other}, device_id_type=pl.DeviceIdType.MESH,
        )

    for b in range(blocks):
        count = min(BLOCK, share - b * BLOCK)
        if count < BLOCK:
            result[...] = jnp.zeros_like(result)

        def wait_block(i, carry):
            block_copy(b, i).wait()
            return carry

        lax.fori_loop(1, n, wait_block, 0)
        pltpu.make_async_copy(spec.at[b, me], recv.at[b, me], own.at[b]).wait()

        def widen(i, carry):
            for s in range(slots):
                wide = recv[b, i, s].astype(F32)
                begin = pl.multiple_of((i * slots + s) * 2 * BLOCK, 8)
                for h in range(halves):
                    gathered[h, pl.ds(begin, 2 * BLOCK), :] = wide[:, h * 128 : (h + 1) * 128]
            return carry

        lax.fori_loop(0, n, widen, 0)

        def wave_step(r, carry):
            wave = owner[me * share + b * BLOCK + r]
            expanded = jnp.dot(
                pick[...].astype(BF16), legendre[b * BLOCK + r], preferred_element_type=F32
            ).astype(BF16)
            pieces = []
            for t in range(2):
                for h in range(halves):
                    piece = gathered[h, pl.ds(t * BLOCK + r, everything, stride=2 * BLOCK), :]
                    pieces.append((piece * quad_slot[...]).astype(BF16))
            weighted = jnp.concatenate(pieces, axis=1)
            coefficient = lax.dot_general(
                expanded, weighted, (((0,), (0,)), ((), ())), preferred_element_type=F32
            )
            kept = degree >= wave
            factor = jnp.where(wave > 0, 2.0, 1.0).astype(F32)
            mixed = []
            for t in range(2):
                part = coefficient[:, t * channels : (t + 1) * channels] * gain[...]
                part = jnp.where(kept, part, 0.0).astype(BF16)
                mixed.append(jnp.dot(part, mix[...], preferred_element_type=F32).astype(BF16))
            synthesis = jnp.dot(
                expanded, jnp.concatenate(mixed, axis=1), preferred_element_type=F32
            ) * factor
            for t in range(2):
                for h in range(halves):
                    begin = t * channels + h * 128
                    result[h, pl.ds(t * BLOCK + r, everything, stride=2 * BLOCK), :] = synthesis[
                        :, begin : begin + 128
                    ]
            return carry

        lax.fori_loop(0, count, wave_step, 0)

        def narrow(i, carry):
            for s in range(slots):
                begin = pl.multiple_of((i * slots + s) * 2 * BLOCK, 8)
                outgoing[b, i, s] = jnp.concatenate(
                    [result[h, pl.ds(begin, 2 * BLOCK), :] for h in range(halves)], axis=1
                ).astype(BF16)
            return carry

        lax.fori_loop(0, n, narrow, 0)

        def start_return(i, carry):
            return_copy(b, i).start()
            return carry

        lax.fori_loop(1, n, start_return, 0)
        pltpu.make_async_copy(outgoing.at[b, me], back.at[b, me], back_own.at[b]).start()

    for b in range(blocks):

        def wait_return(i, carry):
            return_copy(b, i).wait()
            return carry

        lax.fori_loop(1, n, wait_return, 0)
        pltpu.make_async_copy(outgoing.at[b, me], back.at[b, me], back_own.at[b]).wait()


def inverse_kernel(back, table, out):
    block = back[...].reshape(table.shape[1], back.shape[-1])
    out[0] = jnp.dot(table[...], block, preferred_element_type=F32).astype(BF16)


def body(
    n, grid_values, lat_counts, owner_wavenumber, legendre, quad_weight, spectral_gain, channel_mix
):
    slots, longitudes, channels = grid_values.shape
    waves = owner_wavenumber.shape[0]
    share, live_total, degrees = legendre.shape
    blocks = -(-share // BLOCK)
    padded = blocks * BLOCK
    everything = n * slots
    base = jnp.asarray(trig_table(waves, longitudes))
    slot_waves = owner_wavenumber.reshape(n, share)
    slot_waves = jnp.pad(slot_waves, ((0, 0), (0, padded - share)), constant_values=-2 * waves)
    slot_waves = slot_waves.reshape(n, blocks, 1, BLOCK).transpose(1, 0, 2, 3)
    rows = jnp.concatenate([slot_waves, slot_waves + waves], axis=2).reshape(-1, 1)

    vmem = pl.BlockSpec(memory_space=pltpu.VMEM)
    smem = pl.BlockSpec(memory_space=pltpu.SMEM)
    anywhere = pl.BlockSpec(memory_space=pl.ANY)
    limit = 60 * 1024 * 1024
    packet = (blocks, n, slots, 2 * BLOCK, channels)
    copies = pltpu.SemaphoreType.DMA
    back, back_table = pl.pallas_call(
        functools.partial(spectral_kernel, "lat", n, live_total * longitudes, share),
        out_shape=(
            jax.ShapeDtypeStruct(packet, BF16),
            jax.ShapeDtypeStruct((longitudes, blocks * n * 2 * BLOCK), BF16),
        ),
        in_specs=[smem, smem] + [vmem] * 7,
        out_specs=(anywhere, vmem),
        scratch_shapes=[
            pltpu.VMEM((n, 2, channels), F32),
            pltpu.VMEM((blocks * n * 2 * BLOCK, longitudes), BF16),
            pltpu.VMEM((slots, longitudes, channels), BF16),
            pltpu.VMEM(packet, BF16),
            pltpu.VMEM(packet, BF16),
            pltpu.VMEM((channels // 128, everything * 2 * BLOCK, 128), F32),
            pltpu.VMEM((everything, live_total), F32),
            pltpu.VMEM((everything, 128), F32),
            pltpu.VMEM(packet, BF16),
            pltpu.VMEM((channels // 128, everything * 2 * BLOCK, 128), F32),
            copies((n,)), copies((n,)),
            copies((blocks, n)), copies((blocks, n)), copies((blocks,)),
            copies((blocks, n)), copies((blocks, n)), copies((blocks,)),
        ],
        compiler_params=pltpu.CompilerParams(
            collective_id=0, has_side_effects=True, vmem_limit_bytes=limit
        ),
    )(
        lat_counts, owner_wavenumber, grid_values, base, rows, legendre,
        quad_weight.reshape(1, live_total), spectral_gain, channel_mix,
    )

    return pl.pallas_call(
        inverse_kernel,
        grid=(slots,),
        out_shape=jax.ShapeDtypeStruct((slots, longitudes, channels), BF16),
        in_specs=[
            pl.BlockSpec((blocks, n, None, 2 * BLOCK, channels), lambda s: (0, 0, s, 0, 0)),
            pl.BlockSpec((longitudes, blocks * n * 2 * BLOCK), lambda s: (0, 0)),
        ],
        out_specs=pl.BlockSpec((1, longitudes, channels), lambda s: (s, 0, 0)),
        compiler_params=pltpu.CompilerParams(vmem_limit_bytes=limit),
    )(back, back_table)


def solution(mesh):
    return jax.shard_map(
        functools.partial(body, mesh.shape["lat"]),
        mesh=mesh,
        in_specs=(P(("group", "lat"), None, None), P(), P(), P("lat", None, None), P(), P(), P()),
        out_specs=P(("group", "lat"), None, None),
        check_vma=False,
    )
```

```python
import functools
import math

import jax
import jax.numpy as jnp
import numpy as np
from jax import lax
from jax.experimental import pallas as pl
from jax.experimental.pallas import tpu as pltpu
from jax.sharding import PartitionSpec as P

BLOCK = 8
F32 = jnp.float32
BF16 = jnp.bfloat16


def trig_table(waves, longitudes):
    phase = np.arange(waves)[:, None] * np.arange(longitudes)[None, :] % longitudes
    angle = phase * (2.0 * math.pi / longitudes)
    factor = 1.0 / math.sqrt(longitudes)
    table = np.concatenate([np.cos(angle) * factor, -np.sin(angle) * factor], axis=0)
    return table.astype(BF16)


def greet_all(axis, count, me):
    barrier = pltpu.get_barrier_semaphore()

    def signal(i, carry):
        other = lax.rem(me + i, count)
        pl.semaphore_signal(
            barrier, inc=1, device_id={axis: other}, device_id_type=pl.DeviceIdType.MESH
        )
        return carry

    lax.fori_loop(1, count, signal, 0)
    return barrier


def spectral_kernel(
    axis, n, points, share, counts, owner, x, base_far, waves_lane, legendre_far, quad, gain_far,
    mix, last, back_table, partial,
    sums, full, table, front, normed, spec, recv, gathered, pick, quad_slot, outgoing, result,
    early, base, legendre, gain,
    load, fetch, mom_send, mom_recv, send, arrive, own, back_send, back_arrive, back_own, store,
):
    me = lax.axis_index(axis)
    slots, channels = x.shape[0], x.shape[2]
    everything = n * slots
    live_total, degrees = legendre.shape[1], legendre.shape[2]
    halves = channels // 128
    blocks = spec.shape[0]
    lines = n * 2 * BLOCK
    padded = blocks * BLOCK

    def load_slot(s):
        return pltpu.make_async_copy(x.at[s], normed.at[s], load.at[s])

    def start_load(s, carry):
        load_slot(s).start()
        return carry

    lax.fori_loop(0, slots, start_load, 0)
    base_copy = pltpu.make_async_copy(base_far, base, fetch.at[0])
    legendre_copy = pltpu.make_async_copy(legendre_far, legendre, fetch.at[1])
    gain_copy = pltpu.make_async_copy(gain_far, gain, fetch.at[2])
    base_copy.start()
    legendre_copy.start()
    gain_copy.start()
    barrier = greet_all(axis, n, me)
    live = counts[me]
    group = math.gcd(x.shape[1], 32)
    zero = jnp.zeros((group, channels), F32)

    def add_slot(s, carry):
        first, second = carry
        load_slot(s).wait()
        wide = normed[s].astype(F32).reshape(-1, group, channels)
        weight = jnp.where(s < live, 1.0, 0.0).astype(F32)
        first = first + weight * jnp.sum(wide, axis=0)
        second = second + weight * jnp.sum(wide * wide, axis=0)
        return first, second

    first, second = lax.fori_loop(0, slots, add_slot, (zero, zero))
    sums[me, 0:1, :] = jnp.sum(first, axis=0, keepdims=True)
    sums[me, 1:2, :] = jnp.sum(second, axis=0, keepdims=True)
    pl.semaphore_wait(barrier, n - 1)

    def moment_copy(i):
        other = lax.rem(me + i, n)
        return pltpu.make_async_remote_copy(
            src_ref=sums.at[me], dst_ref=sums.at[me],
            send_sem=mom_send.at[i], recv_sem=mom_recv.at[i],
            device_id={axis: other}, device_id_type=pl.DeviceIdType.MESH,
        )

    def start_moment(i, carry):
        moment_copy(i).start()
        return carry

    def wait_moment(i, carry):
        moment_copy(i).wait()
        return carry

    lax.fori_loop(1, n, start_moment, 0)
    waves = base.shape[0] // 2
    natural = lax.broadcasted_iota(jnp.int32, (waves, n * padded), 0)
    chosen = jnp.where(natural == waves_lane[...], 1.0, 0.0).astype(BF16)
    base_copy.wait()
    for t in range(2):
        full[t] = lax.dot_general(
            chosen, base[t * waves : (t + 1) * waves], (((0,), (0,)), ((), ())),
            preferred_element_type=F32,
        )

    def order_rows(o, carry):
        for b in range(blocks):
            begin = pl.multiple_of(o * padded + b * BLOCK, BLOCK)
            both = [full[t, pl.ds(begin, BLOCK), :] for t in range(2)]
            begin = pl.multiple_of((b * n + o) * 2 * BLOCK, 2 * BLOCK)
            table[pl.ds(begin, 2 * BLOCK), :] = jnp.concatenate(both, axis=0).astype(BF16)
        return carry

    lax.fori_loop(0, n, order_rows, 0)
    lax.fori_loop(1, n, wait_moment, 0)
    both = jnp.sum(sums[...], axis=0)
    mean = both[0:1] / points
    variance = both[1:2] / points - mean * mean
    scale = lax.rsqrt(variance + 1e-05)

    def block_copy(b, i):
        other = lax.rem(me + i, n)
        return pltpu.make_async_remote_copy(
            src_ref=spec.at[b, other], dst_ref=recv.at[b, me],
            send_sem=send.at[b, i], recv_sem=arrive.at[b, i],
            device_id={axis: other}, device_id_type=pl.DeviceIdType.MESH,
        )

    for b in range(blocks):

        def slot_step(s, carry):
            if b == 0:
                weight = jnp.where(s < live, 1.0, 0.0).astype(F32)
                normed[s] = ((normed[s].astype(F32) - mean) * scale * weight).astype(BF16)
            out = jnp.dot(
                table[b * lines : (b + 1) * lines], normed[s], preferred_element_type=F32
            )
            spec[b, :, s] = out.astype(BF16).reshape(n, 2 * BLOCK, channels)
            if b == 0:

                def start_slot(i, inner):
                    other = lax.rem(me + i, n)
                    pltpu.make_async_remote_copy(
                        src_ref=spec.at[b, other, s], dst_ref=recv.at[b, me, s],
                        send_sem=send.at[b, i], recv_sem=arrive.at[b, i],
                        device_id={axis: other}, device_id_type=pl.DeviceIdType.MESH,
                    ).start()
                    return inner

                lax.fori_loop(1, n, start_slot, 0)
            return carry

        lax.fori_loop(0, slots, slot_step, 0)
        if b > 0:

            def start_block(i, carry):
                block_copy(b, i).start()
                return carry

            lax.fori_loop(1, n, start_block, 0)
        pltpu.make_async_copy(spec.at[b, me], recv.at[b, me], own.at[b]).start()

    late = (blocks - 1) * lines
    back_table[...] = table[late:].T
    if blocks > 1:
        front[...] = table[:late].T
    legendre_copy.wait()
    gain_copy.wait()
    row = lax.broadcasted_iota(jnp.int32, (everything, live_total), 0)
    lane = lax.broadcasted_iota(jnp.int32, (everything, live_total), 1)
    pick[...] = jnp.zeros_like(pick)

    def mark(i, begin):
        within = row - i * slots
        hit = (within >= 0) & (within < counts[i]) & (lane == begin + within)
        pick[...] += jnp.where(hit, 1.0, 0.0).astype(F32)
        return begin + counts[i]

    lax.fori_loop(0, n, mark, jnp.int32(0))
    quad_slot[...] = jnp.broadcast_to(
        jnp.sum(pick[...] * quad[...], axis=1, keepdims=True), quad_slot.shape
    )
    degree = lax.broadcasted_iota(jnp.int32, (degrees, channels), 0)

    def landing(b):
        return early.at[b, me] if b < blocks - 1 else last.at[me]

    def return_copy(b, i):
        other = lax.rem(me + i, n)
        return pltpu.make_async_remote_copy(
            src_ref=outgoing.at[b, other], dst_ref=landing(b),
            send_sem=back_send.at[b, i], recv_sem=back_arrive.at[b, i],
            device_id={axis: other}, device_id_type=pl.DeviceIdType.MESH,
        )

    for b in range(blocks):
        count = min(BLOCK, share - b * BLOCK)
        if count < BLOCK:
            result[...] = jnp.zeros_like(result)

        def wait_block(i, carry):
            block_copy(b, i).wait()
            return carry

        lax.fori_loop(1, n, wait_block, 0)
        pltpu.make_async_copy(spec.at[b, me], recv.at[b, me], own.at[b]).wait()

        def widen(i, carry):
            for s in range(slots):
                wide = recv[b, i, s].astype(F32)
                begin = pl.multiple_of((i * slots + s) * 2 * BLOCK, 8)
                for h in range(halves):
                    gathered[h, pl.ds(begin, 2 * BLOCK), :] = wide[:, h * 128 : (h + 1) * 128]
            return carry

        lax.fori_loop(0, n, widen, 0)

        def wave_step(r, carry):
            wave = owner[me * share + b * BLOCK + r]
            expanded = jnp.dot(
                pick[...].astype(BF16), legendre[b * BLOCK + r], preferred_element_type=F32
            ).astype(BF16)
            pieces = []
            for t in range(2):
                for h in range(halves):
                    piece = gathered[h, pl.ds(t * BLOCK + r, everything, stride=2 * BLOCK), :]
                    pieces.append((piece * quad_slot[...]).astype(BF16))
            weighted = jnp.concatenate(pieces, axis=1)
            coefficient = lax.dot_general(
                expanded, weighted, (((0,), (0,)), ((), ())), preferred_element_type=F32
            )
            kept = degree >= wave
            factor = jnp.where(wave > 0, 2.0, 1.0).astype(F32)
            mixed = []
            for t in range(2):
                part = coefficient[:, t * channels : (t + 1) * channels] * gain[...]
                part = jnp.where(kept, part, 0.0).astype(BF16)
                mixed.append(jnp.dot(part, mix[...], preferred_element_type=F32).astype(BF16))
            synthesis = jnp.dot(
                expanded, jnp.concatenate(mixed, axis=1), preferred_element_type=F32
            ) * factor
            for t in range(2):
                for h in range(halves):
                    begin = t * channels + h * 128
                    result[h, pl.ds(t * BLOCK + r, everything, stride=2 * BLOCK), :] = synthesis[
                        :, begin : begin + 128
                    ]
            return carry

        lax.fori_loop(0, count, wave_step, 0)

        def narrow(i, carry):
            for s in range(slots):
                begin = pl.multiple_of((i * slots + s) * 2 * BLOCK, 8)
                outgoing[b, i, s] = jnp.concatenate(
                    [result[h, pl.ds(begin, 2 * BLOCK), :] for h in range(halves)], axis=1
                ).astype(BF16)
            return carry

        lax.fori_loop(0, n, narrow, 0)

        def start_return(i, carry):
            return_copy(b, i).start()
            return carry

        lax.fori_loop(1, n, start_return, 0)
        pltpu.make_async_copy(outgoing.at[b, me], landing(b), back_own.at[b]).start()

    def settle(b):
        def wait_return(i, carry):
            return_copy(b, i).wait()
            return carry

        lax.fori_loop(1, n, wait_return, 0)
        pltpu.make_async_copy(outgoing.at[b, me], landing(b), back_own.at[b]).wait()

    def store_slot(s):
        return pltpu.make_async_copy(normed.at[s], partial.at[s], store.at[s])

    for b in range(blocks - 1):
        settle(b)

    def partial_slot(s, carry):
        if blocks > 1:
            block = early[:, :, s].reshape(late, channels)
            normed[s] = jnp.dot(front[...], block, preferred_element_type=F32).astype(BF16)
        else:
            normed[s] = jnp.zeros(normed.shape[1:], BF16)
        store_slot(s).start()
        return carry

    def wait_store(s, carry):
        store_slot(s).wait()
        return carry

    lax.fori_loop(0, slots, partial_slot, 0)
    lax.fori_loop(0, slots, wait_store, 0)
    settle(blocks - 1)


def inverse_kernel(last, table, partial, out):
    block = last[...].reshape(table.shape[1], last.shape[-1])
    total = jnp.dot(table[...], block, preferred_element_type=F32)
    out[0] = (partial[0].astype(F32) + total).astype(BF16)


def body(
    n, grid_values, lat_counts, owner_wavenumber, legendre, quad_weight, spectral_gain, channel_mix
):
    slots, longitudes, channels = grid_values.shape
    waves = owner_wavenumber.shape[0]
    share, live_total, degrees = legendre.shape
    blocks = -(-share // BLOCK)
    padded = blocks * BLOCK
    everything = n * slots
    base = jnp.asarray(trig_table(waves, longitudes))
    slot_waves = owner_wavenumber.reshape(n, share)
    slot_waves = jnp.pad(slot_waves, ((0, 0), (0, padded - share)), constant_values=-1)
    waves_lane = slot_waves.reshape(1, n * padded)

    vmem = pl.BlockSpec(memory_space=pltpu.VMEM)
    smem = pl.BlockSpec(memory_space=pltpu.SMEM)
    anywhere = pl.BlockSpec(memory_space=pl.ANY)
    limit = 60 * 1024 * 1024
    packet = (blocks, n, slots, 2 * BLOCK, channels)
    copies = pltpu.SemaphoreType.DMA
    lines = n * 2 * BLOCK
    last, back_table, partial = pl.pallas_call(
        functools.partial(spectral_kernel, "lat", n, live_total * longitudes, share),
        out_shape=(
            jax.ShapeDtypeStruct(packet[1:], BF16),
            jax.ShapeDtypeStruct((longitudes, lines), BF16),
            jax.ShapeDtypeStruct((slots, longitudes, channels), BF16),
        ),
        in_specs=[smem, smem, anywhere, anywhere, vmem, anywhere, vmem, anywhere, vmem],
        out_specs=(anywhere, vmem, anywhere),
        scratch_shapes=[
            pltpu.VMEM((n, 2, channels), F32),
            pltpu.VMEM((2, n * padded, longitudes), F32),
            pltpu.VMEM((blocks * lines, longitudes), BF16),
            pltpu.VMEM((longitudes, max(blocks - 1, 1) * lines), BF16),
            pltpu.VMEM((slots, longitudes, channels), BF16),
            pltpu.VMEM(packet, BF16),
            pltpu.VMEM(packet, BF16),
            pltpu.VMEM((channels // 128, everything * 2 * BLOCK, 128), F32),
            pltpu.VMEM((everything, live_total), F32),
            pltpu.VMEM((everything, 128), F32),
            pltpu.VMEM(packet, BF16),
            pltpu.VMEM((channels // 128, everything * 2 * BLOCK, 128), F32),
            pltpu.VMEM((max(blocks - 1, 1),) + packet[1:], BF16),
            pltpu.VMEM(base.shape, BF16),
            pltpu.VMEM(legendre.shape, BF16),
            pltpu.VMEM(spectral_gain.shape, F32),
            copies((slots,)), copies((3,)),
            copies((n,)), copies((n,)),
            copies((blocks, n)), copies((blocks, n)), copies((blocks,)),
            copies((blocks, n)), copies((blocks, n)), copies((blocks,)),
            copies((slots,)),
        ],
        compiler_params=pltpu.CompilerParams(
            collective_id=0, has_side_effects=True, vmem_limit_bytes=limit
        ),
    )(
        lat_counts, owner_wavenumber, grid_values, base, waves_lane, legendre,
        quad_weight.reshape(1, live_total), spectral_gain, channel_mix,
    )

    return pl.pallas_call(
        inverse_kernel,
        grid=(slots,),
        out_shape=jax.ShapeDtypeStruct((slots, longitudes, channels), BF16),
        in_specs=[
            pl.BlockSpec((n, None, 2 * BLOCK, channels), lambda s: (0, s, 0, 0)),
            pl.BlockSpec((longitudes, lines), lambda s: (0, 0)),
            pl.BlockSpec((1, longitudes, channels), lambda s: (s, 0, 0)),
        ],
        out_specs=pl.BlockSpec((1, longitudes, channels), lambda s: (s, 0, 0)),
        compiler_params=pltpu.CompilerParams(vmem_limit_bytes=limit),
    )(last, back_table, partial)


def solution(mesh):
    return jax.shard_map(
        functools.partial(body, mesh.shape["lat"]),
        mesh=mesh,
        in_specs=(P(("group", "lat"), None, None), P(), P(), P("lat", None, None), P(), P(), P()),
        out_specs=P(("group", "lat"), None, None),
        check_vma=False,
    )
```
